512 devices in a mesh: groups: 2 (over y), req: 16 (over z), head: 8 (over x), sub: 2 (over core).
Axes of the slice: x: 8, y: 2, z: 16, core: 2. Of those that a mesh axis runs over, the one named last changes fastest.
The devices are a block of a 8x8x16 slice.
Arguments:
- q_nope: bfloat16 [8192, 8192], P(('groups', 'req', 'sub'), 'head'), parts along dimension 0, may hold values from -12 to 12
- q_rope: bfloat16 [8192, 4096], P(('groups', 'req', 'sub'), 'head'), parts along dimension 0, may hold values from -16 to 16
- new_latent: bfloat16 [8192, 512], P(('groups', 'req', 'sub')), parts along dimension 0, may hold values from -6 to 6
- new_rope: bfloat16 [8192, 64], P(('groups', 'req', 'sub')), parts along dimension 0, may hold values from -8 to 8
- pool_latent: bfloat16 [512, 128, 512], P(('groups', 'req'), None, 'sub'), parts along dimension 0, may hold values from -6 to 6
- pool_rope: bfloat16 [512, 128, 64], P(('groups', 'req')), parts along dimension 0, may hold values from -6 to 6
- w_uk: bfloat16 [512, 8192], P(None, 'head'), may hold values from -0.25 to 0.25
- w_uv: bfloat16 [512, 8192], P(None, 'head'), may hold values from -0.25 to 0.25
- block_list: int32 [32, 6], P(('groups', 'req')), parts along dimension 0, may hold values from 0 to 255, as said below
- prefix_len: int32 [32], P(('groups', 'req')), parts along dimension 0, may hold values from 192 to 768, as said below
- block_slot: int32 [512], P('groups'), parts along dimension 0, may hold values from 0 to 255, as said below
Outputs:
- attended: bfloat16 [8192, 8192], P(('groups', 'req', 'sub'), 'head'), parts along dimension 0
The draws below stay inside these ranges and needn't reach their ends.
There are 2 independent parts, one for each index of `groups`. The reference program is written for one: setup_inputs(seed, part) draws one part's arguments, and reference() takes and returns one part's arrays. A program takes and returns all parts, laid end to end along the dimension named above; an argument that names none is the same for every part. Nothing has to cross between parts.
Inputs may be any that keep to these rules, and one draw needn't show every extreme that they name: `block_list`: each row lists 6 different block ids; no row lists more than 2 blocks stored with one owner (storage positions o * 16 to o * 16 + 15), and in every draw some owner stores 2 blocks of every row. `prefix_len`: some row has the full 6 * 128 prefix tokens. `block_slot`: each storage position once.
All inputs are finite; a program needn't handle non-finite values.
Results may differ from the reference program's by a relative error of at most 0.0072.
Values may be sent and summed in bfloat16 or wider, within the bound.
A program may use at most 64 MiB of HBM per device.

```python
import math
import jax
import jax.numpy as jnp
from jax import lax

HEADS = 64
NOPE = 128
ROPE = 64
VDIM = 128
LATENT = 512
BLOCK = 128
CAP = 2
POOL_DEV = 16
QUERIES = 256
PB = 6
ROWS = 16
POOL = 256


def draw_q_rope(key, part):
    kbase = jax.random.fold_in(key, 3)
    base = jnp.clip(2.0 * jax.random.normal(kbase, (ROWS * QUERIES, HEADS * ROPE), jnp.float32), -16.0, 16.0)
    return base.astype(jnp.bfloat16)


def draw_new_rope(key, part):
    kbase = jax.random.fold_in(key, 5)
    base = jnp.clip(jax.random.normal(kbase, (ROWS * QUERIES, ROPE), jnp.float32), -8.0, 8.0)
    return base.astype(jnp.bfloat16)


def draw_prefix_len(key, part):
    klen, kpick = jax.random.split(jax.random.fold_in(key, 11))
    full = PB * BLOCK
    lengths = jax.random.randint(klen, (ROWS,), full // 4, full + 1)
    pick = jax.random.randint(kpick, (), 0, ROWS)
    return lengths.at[pick].set(full).astype(jnp.int32)


def block_tables(key):
    kperm, khot, krows = jax.random.split(jax.random.fold_in(key, 23), 3)
    slots = jax.random.permutation(kperm, POOL)
    inverse = jnp.argsort(slots)
    hot = jax.random.randint(khot, (), 0, ROWS)
    rest = jnp.arange((ROWS - 1) * CAP)
    other_owner = rest // CAP
    other_owner = other_owner + (other_owner >= hot).astype(other_owner.dtype)
    other_copy = rest % CAP

    def one_row(rowkey):
        kpick, kshuf, kbase = jax.random.split(rowkey, 3)
        chosen = jax.random.permutation(kpick, (ROWS - 1) * CAP)[:PB - CAP]
        owner = jnp.concatenate([jnp.full((CAP,), hot, other_owner.dtype), other_owner[chosen]])
        copies = jnp.concatenate([jnp.arange(CAP, dtype=other_copy.dtype), other_copy[chosen]])
        shuffle = jax.random.permutation(kshuf, PB)
        owner = owner[shuffle]
        copies = copies[shuffle]
        base = jax.random.randint(kbase, (ROWS,), 0, POOL_DEV)
        local = (base[owner] + copies) % POOL_DEV
        return inverse[owner * POOL_DEV + local]
    lists = jax.vmap(one_row)(jax.random.split(krows, ROWS))
    return (lists.astype(jnp.int32), slots.astype(jnp.int32))


def draw_block_list(key, part):
    return block_tables(key)[0]


def draw_block_slot(key, part):
    return block_tables(key)[1]


def block_levels(stream_key, shape, shards, low, top_value):
    def one(dim, parts):
        heights = jax.random.uniform(jax.random.fold_in(jax.random.fold_in(stream_key, 6), dim), (parts,), jnp.float32, low / len(shards), top_value / len(shards))
        return jnp.repeat(jnp.exp(heights), shape[dim] // parts).reshape((-1,) + (1,) * (len(shape) - dim - 1))

    level = one(*shards[0])
    for cut in shards[1:]:
        level = level * one(*cut)
    return level


def normal_values(rng, extent, width, most, cuts=(), kind=jnp.bfloat16):
    result = width * jax.random.normal(rng, extent, jnp.float32)
    if cuts:
        result = result * block_levels(rng, extent, cuts, -0.22, 0.18)
    return jnp.clip(result, -most, most).astype(kind)


def setup_inputs(seed: int = 0, part: int = 0) -> dict:
    keys = jax.random.split(jax.random.key(seed), 12)
    part_splits = jax.random.split(jax.random.fold_in(keys[11], part), 12)
    q_nope = normal_values(part_splits[0], (ROWS * QUERIES, HEADS * NOPE), 2.0, 12.0, ((0, 32), (1, 8)))
    q_rope = draw_q_rope(jax.random.fold_in(jax.random.fold_in(keys[11], part), 71), part)
    new_latent = normal_values(part_splits[2], (ROWS * QUERIES, LATENT), 1.0, 6.0, ((0, 32),))
    new_rope = draw_new_rope(jax.random.fold_in(jax.random.fold_in(keys[11], part), 71), part)
    pool_latent = normal_values(part_splits[4], (POOL, BLOCK, LATENT), 1.0, 6.0, ((0, 16), (2, 2)))
    pool_rope = normal_values(part_splits[5], (POOL, BLOCK, ROPE), 1.0, 6.0, ((0, 16),))
    w_uk = normal_values(keys[6], (LATENT, HEADS * NOPE), LATENT ** -0.5, 0.25, ((1, 8),))
    w_uv = normal_values(keys[7], (LATENT, HEADS * VDIM), LATENT ** -0.5, 0.25, ((1, 8),))
    block_list = draw_block_list(jax.random.fold_in(jax.random.fold_in(keys[11], part), 71), part)
    prefix_len = draw_prefix_len(jax.random.fold_in(jax.random.fold_in(keys[11], part), 71), part)
    block_slot = draw_block_slot(jax.random.fold_in(jax.random.fold_in(keys[11], part), 71), part)
    return dict(q_nope=q_nope, q_rope=q_rope, new_latent=new_latent, new_rope=new_rope, pool_latent=pool_latent, pool_rope=pool_rope, w_uk=w_uk, w_uv=w_uv, block_list=block_list, prefix_len=prefix_len, block_slot=block_slot)


def reference(q_nope, q_rope, new_latent, new_rope, pool_latent, pool_rope, w_uk, w_uv, block_list, prefix_len, block_slot):
    scale = 1.0 / math.sqrt(NOPE + ROPE)
    prefix = PB * BLOCK
    total = prefix + QUERIES

    def one_row(row):
        physical = block_slot[block_list[row]]
        lat = pool_latent[physical].reshape(prefix, LATENT)
        rope = pool_rope[physical].reshape(prefix, ROPE)
        start = (row * QUERIES).astype(jnp.int32)
        fresh_lat = lax.dynamic_slice_in_dim(new_latent, start, QUERIES, 0)
        fresh_rope = lax.dynamic_slice_in_dim(new_rope, start, QUERIES, 0)
        key_latent = jnp.concatenate([lat, fresh_lat], axis=0)
        key_rope = jnp.concatenate([rope, fresh_rope], axis=0)
        key_nope = jnp.dot(key_latent, w_uk, preferred_element_type=jnp.float32).astype(jnp.bfloat16).reshape(total, HEADS, NOPE)
        values = jnp.dot(key_latent, w_uv, preferred_element_type=jnp.float32).astype(jnp.bfloat16).reshape(total, HEADS, VDIM)
        query_nope = lax.dynamic_slice_in_dim(q_nope, start, QUERIES, 0).reshape(QUERIES, HEADS, NOPE)
        query_rope = lax.dynamic_slice_in_dim(q_rope, start, QUERIES, 0).reshape(QUERIES, HEADS, ROPE)
        scores = jnp.einsum('qhd,khd->hqk', query_nope.astype(jnp.float32), key_nope.astype(jnp.float32))
        scores = scores + jnp.einsum('qhd,kd->hqk', query_rope.astype(jnp.float32), key_rope.astype(jnp.float32))
        scores = scores * scale
        key_pos = jnp.arange(total, dtype=jnp.int32)
        query_pos = jnp.arange(QUERIES, dtype=jnp.int32)
        visible = jnp.where(key_pos[None, :] < prefix, key_pos[None, :] < prefix_len[row], key_pos[None, :] - prefix <= query_pos[:, None])
        scores = jnp.where(visible[None], scores, jnp.float32(-1e+30))
        peak = lax.optimization_barrier(jnp.max(scores, axis=2, keepdims=True))
        expo = jnp.where(visible[None], jnp.exp(scores - peak), jnp.float32(0.0))
        weights = (expo / lax.optimization_barrier(jnp.sum(expo, axis=2, keepdims=True))).astype(jnp.bfloat16)
        out = jnp.einsum('hqk,khd->qhd', weights.astype(jnp.float32), values.astype(jnp.float32))
        return out.astype(jnp.bfloat16).reshape(QUERIES, HEADS * VDIM)
    outs = lax.map(one_row, jnp.arange(ROWS, dtype=jnp.int32))
    return outs.reshape(ROWS * QUERIES, HEADS * VDIM)
```

```python
import functools
import math

import jax
import jax.numpy as jnp
from jax import lax
from jax.experimental import pallas as pl
from jax.experimental.pallas import tpu as pltpu
from jax.sharding import PartitionSpec as P

NOPE = 128
ROPE = 64
VDIM = 128
CAP = 2
MESH = pl.DeviceIdType.MESH
BF = jnp.bfloat16
F32 = jnp.float32


def exchange(
    blocks,
    pool_local,
    list_ref,
    slot_ref,
    pool_lat,
    pool_rope,
    new_lat,
    new_rope,
    lat_mine,
    lat_other,
    rope_mine,
    rope_other,
    new_lat_other,
    new_rope_other,
    pool_l,
    pool_r,
    send_l,
    send_r,
    got_l,
    got_r,
    own_v,
    table_in,
    table_out,
    asked_v,
    table_s,
    asked_s,
    pool_sem,
    small_sem,
    hello_sem,
    table_sem,
    ask_send,
    ask_recv,
    lat_send,
    lat_recv,
    rope_send,
    rope_recv,
    xlat_send,
    xlat_recv,
    xrope_send,
    xrope_recv,
    slat_send,
    slat_recv,
    srope_send,
    srope_recv,
    snew_send,
    snew_recv,
):
    rows = lax.axis_size("req")
    heads = lax.axis_size("head")
    row = lax.axis_index("req")
    lane = lax.axis_index("head")
    core = lax.axis_index("sub")
    other = {"sub": 1 - core}
    carriers = heads // 2
    tokens = pool_l.shape[1]
    feats = pool_r.shape[1]
    part = lane // 2
    carrier = lax.rem(lane, 2) == 1
    token_at = pl.multiple_of(part * tokens, tokens)
    feat_at = pl.multiple_of(part * feats, feats)
    barrier = pltpu.get_barrier_semaphore()

    for step in range(1, heads):
        pl.semaphore_signal(
            barrier, inc=1, device_id={"head": lax.rem(lane + step, heads)}, device_id_type=MESH
        )
    pl.semaphore_signal(barrier, inc=1, device_id=other, device_id_type=MESH)

    @pl.when(carrier)
    def _():
        def tell(p, carry):
            pl.semaphore_signal(barrier, inc=1, device_id={"req": p}, device_id_type=MESH)
            return carry

        lax.fori_loop(row + 1, rows, tell, 0)

    load_l = pltpu.make_async_copy(
        pool_lat.at[:, pl.ds(token_at, tokens), :], pool_l, pool_sem.at[0]
    )
    load_r = pltpu.make_async_copy(
        pool_rope.at[:, pl.ds(feat_at, feats), :], pool_r, pool_sem.at[1]
    )

    @pl.when(carrier)
    def _():
        load_l.start()
        load_r.start()

    physical = [slot_ref[list_ref[0, j]] for j in range(blocks)]
    column = lax.broadcasted_iota(jnp.int32, own_v.shape, 1)
    own = jnp.zeros(own_v.shape, jnp.int32)
    for j in range(blocks):
        own = jnp.where(column == j, physical[j], own)
    own_v[...] = own

    @pl.when(row > 0)
    def _():
        pl.semaphore_wait(barrier, heads + jnp.where(carrier, row, 0))

    def lat_copy(p, sem_at):
        return pltpu.make_async_remote_copy(
            send_l.at[p], got_l.at[row], lat_send.at[p], lat_recv.at[sem_at], {"req": p}, MESH
        )

    def rope_copy(p, sem_at):
        return pltpu.make_async_remote_copy(
            send_r.at[p], got_r.at[row], rope_send.at[p], rope_recv.at[sem_at], {"req": p}, MESH
        )

    def ask_copy(p):
        return pltpu.make_async_remote_copy(
            own_v, asked_v.at[row], ask_send.at[p], ask_recv.at[row], {"req": p}, MESH
        )

    def chosen(read):
        count = jnp.int32(0)
        first = jnp.int32(0)
        second = jnp.int32(0)
        for j in range(blocks):
            where = read(j)
            here = (where // pool_local) == row
            local = where - row * pool_local
            first = jnp.where(here & (count == 0), local, first)
            second = jnp.where(here & (count == 1), local, second)
            count = count + here.astype(jnp.int32)
        return first, second

    def serve(p, read):
        first, second = chosen(read)
        send_l[p, 0] = pool_l[first]
        send_l[p, 1] = pool_l[second]
        send_r[p] = pool_r[jnp.where(core == 0, first, second)]
        lat_copy(p, row).start()
        rope_copy(p, row).start()

    table_copy = pltpu.make_async_remote_copy(
        table_out, table_in, table_sem.at[0], table_sem.at[1], {"req": lax.rem(row + 1, rows)}, MESH
    )

    @pl.when(carrier)
    def _():
        @pl.when(row > 0)
        def _():
            pl.semaphore_signal(
                hello_sem, inc=1, device_id={"req": row - 1}, device_id_type=MESH
            )

        def ask(p, carry):
            ask_copy(p).start()
            return carry

        lax.fori_loop(0, row, ask, 0)
        load_l.wait()
        load_r.wait()

        @pl.when(row > 0)
        def _():
            table_copy.wait_recv()
            to_s = pltpu.make_async_copy(table_in, table_s, small_sem.at[0])
            to_s.start()
            to_s.wait()

            def below(p, carry):
                serve(p, lambda j: table_s[p, j])
                return carry

            lax.fori_loop(0, row, below, 0)

        @pl.when(row < rows - 1)
        def _():
            line = lax.broadcasted_iota(jnp.int32, table_out.shape, 0)
            mine = jnp.broadcast_to(own_v[0:1, :], table_out.shape)
            known = jnp.where(line < row, table_in[...], 0)
            table_out[...] = jnp.where(line == row, mine, known)
            pl.semaphore_wait(hello_sem, 1)
            table_copy.start()

            def above(p, carry):
                pltpu.make_async_remote_copy(
                    own_v, asked_v.at[p], ask_send.at[p], ask_recv.at[p], {"req": p}, MESH
                ).wait_recv()
                to_s = pltpu.make_async_copy(asked_v.at[p], asked_s, small_sem.at[1])
                to_s.start()
                to_s.wait()
                serve(p, lambda j: asked_s[0, j])
                return carry

            lax.fori_loop(row + 1, rows, above, 0)

        first, second = chosen(lambda j: physical[j])
        got_l[row, 0] = pool_l[first]
        got_l[row, 1] = pool_l[second]
        got_r[row] = pool_r[jnp.where(core == 0, first, second)]

        def arrived(p, carry):
            @pl.when(p != row)
            def _():
                lat_copy(p, p).wait_recv()
                rope_copy(p, p).wait_recv()

            return carry

        lax.fori_loop(0, rows, arrived, 0)

        for j in range(blocks):
            owner = physical[j] // pool_local
            rank = jnp.int32(0)
            for i in range(j):
                rank = rank + (physical[i] // pool_local == owner).astype(jnp.int32)
            lat_mine[j, pl.ds(token_at, tokens), :] = got_l[owner, jnp.minimum(rank, CAP - 1)]
            piece = got_r[owner]
            rope_mine[j, pl.ds(feat_at, feats), :] = jnp.where(
                rank == core, piece, jnp.zeros_like(piece)
            )

    @pl.when(row == 0)
    def _():
        pl.semaphore_wait(barrier, heads)

    new_copies = [
        pltpu.make_async_remote_copy(
            src, dst, snew_send.at[i], snew_recv.at[i], other, MESH
        )
        for i, (src, dst) in enumerate(((new_lat, new_lat_other), (new_rope, new_rope_other)))
    ]
    for copy in new_copies:
        copy.start()

    def lat_piece(k):
        return pl.ds(pl.multiple_of(k * tokens, tokens), tokens)

    def rope_piece(k):
        return pl.ds(pl.multiple_of(k * feats, feats), feats)

    def xlat_copy(k, peer):
        at = lat_piece(k)
        return pltpu.make_async_remote_copy(
            lat_mine.at[:, at, :],
            lat_mine.at[:, at, :],
            xlat_send.at[peer],
            xlat_recv.at[k],
            {"head": peer},
            MESH,
        )

    def xrope_copy(k, peer):
        at = rope_piece(k)
        return pltpu.make_async_remote_copy(
            rope_mine.at[:, at, :],
            rope_mine.at[:, at, :],
            xrope_send.at[peer],
            xrope_recv.at[k],
            {"head": peer},
            MESH,
        )

    def sub_copies(k):
        at, fat = lat_piece(k), rope_piece(k)
        return (
            pltpu.make_async_remote_copy(
                lat_mine.at[:, at, :],
                lat_other.at[:, at, :],
                slat_send.at[k],
                slat_recv.at[k],
                other,
                MESH,
            ),
            pltpu.make_async_remote_copy(
                rope_mine.at[:, fat, :],
                rope_other.at[:, fat, :],
                srope_send.at[k],
                srope_recv.at[k],
                other,
                MESH,
            ),
        )

    order = [0]
    for step in range(heads // 2, 0, -1):
        for peer in (step, heads - step):
            if peer not in order:
                order.append(peer)
    order = order[1:]

    @pl.when(carrier)
    def _():
        for step in order:
            peer = lax.rem(lane + step, heads)
            xlat_copy(part, peer).start()
            xrope_copy(part, peer).start()
        for copy in sub_copies(part):
            copy.start()

    for k in range(carriers):
        mine = carrier & (part == k)

        @pl.when(jnp.logical_not(mine))
        def _(k=k):
            xlat_copy(k, lane).wait_recv()
            xrope_copy(k, lane).wait_recv()
            for copy in sub_copies(k):
                copy.start()

    for k in range(carriers):
        for copy in sub_copies(k):
            copy.wait()
    for copy in new_copies:
        copy.wait()

    @pl.when(carrier)
    def _():
        for step in order:
            peer = lax.rem(lane + step, heads)
            xlat_copy(part, peer).wait_send()
            xrope_copy(part, peer).wait_send()

        def sent(p, carry):
            @pl.when(p != row)
            def _():
                lat_copy(p, row).wait_send()
                rope_copy(p, row).wait_send()

            @pl.when(p < row)
            def _():
                ask_copy(p).wait_send()

            return carry

        lax.fori_loop(0, rows, sent, 0)

        @pl.when(row < rows - 1)
        def _():
            table_copy.wait_send()


def attend(
    scale,
    length_ref,
    q_nope,
    q_rope,
    lat_mine,
    lat_other,
    rope_mine,
    rope_other,
    new_lat,
    new_lat_other,
    new_rope,
    new_rope_other,
    w_uk,
    w_uv,
    out,
    keys,
    rope_even,
    rope_odd,
    bias,
):
    core = lax.axis_index("sub")
    blocks, block, half = lat_mine.shape
    prefix = blocks * block
    queries = q_nope.shape[0]
    total = keys.shape[0]
    here = pl.ds(pl.multiple_of(core * half, half), half)
    there = pl.ds(pl.multiple_of((1 - core) * half, half), half)
    for j in range(blocks):
        keys[pl.ds(j * block, block), here] = lat_mine[j]
        keys[pl.ds(j * block, block), there] = lat_other[j]
    keys[pl.ds(prefix, queries), :] = new_lat[...]
    keys[pl.ds(prefix + queries, queries), :] = new_lat_other[...]

    def put_rope(at, piece):
        turned = piece.astype(F32).T.astype(BF)
        blank = jnp.zeros_like(turned)
        rope_even[pl.ds(at, turned.shape[0]), :] = jnp.concatenate([turned, blank], axis=1)
        rope_odd[pl.ds(at, turned.shape[0]), :] = jnp.concatenate([blank, turned], axis=1)

    for j in range(blocks):
        put_rope(j * block, rope_mine[j] + rope_other[j])
    put_rope(prefix, new_rope[...])
    put_rope(prefix + queries, new_rope_other[...])

    key = lax.broadcasted_iota(jnp.int32, (queries, total), 1)
    query = lax.broadcasted_iota(jnp.int32, (queries, total), 0)
    last = jnp.where(core == 1, total, prefix + queries)
    hidden = F32(-1e30)
    in_prefix = jnp.where(key < length_ref[0], F32(0.0), hidden)
    in_mine = jnp.where(key - prefix <= query, F32(0.0), hidden)
    in_other = jnp.where(key < last, F32(0.0), hidden)
    fresh = jnp.where(key < prefix + queries, in_mine, in_other)
    bias[...] = jnp.where(key < prefix, in_prefix, fresh)

    def pair(i, carry):
        cols = pl.ds(pl.multiple_of(i * 2 * NOPE, 2 * NOPE), 2 * NOPE)
        k2 = jnp.dot(keys[...], w_uk[:, cols], preferred_element_type=F32).astype(BF)
        v2 = jnp.dot(keys[...], w_uv[:, cols], preferred_element_type=F32).astype(BF)
        qr = q_rope[:, pl.ds(pl.multiple_of(i * 2 * ROPE, 2 * ROPE), 2 * ROPE)]
        qn = q_nope[:, cols]
        outs = []
        for e, kr in ((0, rope_even), (1, rope_odd)):
            kcat = jnp.concatenate([k2[:, e * NOPE : (e + 1) * NOPE], kr[...]], axis=1)
            qcat = jnp.concatenate([qn[:, e * NOPE : (e + 1) * NOPE], qr], axis=1)
            s = lax.dot_general(
                qcat, kcat, (((1,), (1,)), ((), ())), preferred_element_type=F32
            )
            s = s * scale + bias[...]
            peak = jnp.max(s, axis=1, keepdims=True)
            expo = jnp.exp(s - peak)
            weights = (expo * (1.0 / jnp.sum(expo, axis=1, keepdims=True))).astype(BF)
            outs.append(
                jnp.dot(
                    weights, v2[:, e * VDIM : (e + 1) * VDIM], preferred_element_type=F32
                ).astype(BF)
            )
        out[:, cols] = jnp.concatenate(outs, axis=1)
        return carry

    lax.fori_loop(0, q_nope.shape[1] // (2 * NOPE), pair, 0)


def shards(
    q_nope,
    q_rope,
    new_latent,
    new_rope,
    pool_latent,
    pool_rope,
    w_uk,
    w_uv,
    block_list,
    prefix_len,
    block_slot,
):
    rows = lax.axis_size("req")
    heads = lax.axis_size("head")
    pool_local, block, half = pool_latent.shape
    blocks = block_list.shape[1]
    queries = q_nope.shape[0]
    carriers = heads // 2
    tokens = block // carriers
    feats = ROPE // carriers
    pool_rope = jnp.swapaxes(pool_rope, 1, 2)
    new_rope = new_rope.T
    vmem = pl.BlockSpec(memory_space=pltpu.VMEM)
    smem = pl.BlockSpec(memory_space=pltpu.SMEM)
    hbm = pl.BlockSpec(memory_space=pl.ANY)
    dma = pltpu.SemaphoreType.DMA
    shape = jax.ShapeDtypeStruct
    lat_mine, lat_other, rope_mine, rope_other, new_lat_other, new_rope_other = pl.pallas_call(
        functools.partial(exchange, blocks, pool_local),
        out_shape=(
            shape((blocks, block, half), BF),
            shape((blocks, block, half), BF),
            shape((blocks, ROPE, block), BF),
            shape((blocks, ROPE, block), BF),
            shape(new_latent.shape, BF),
            shape(new_rope.shape, BF),
        ),
        in_specs=[smem, smem, hbm, hbm, vmem, vmem],
        out_specs=(vmem,) * 6,
        scratch_shapes=[
            pltpu.VMEM((pool_local, tokens, half), BF),
            pltpu.VMEM((pool_local, feats, block), BF),
            pltpu.VMEM((rows, CAP, tokens, half), BF),
            pltpu.VMEM((rows, feats, block), BF),
            pltpu.VMEM((rows, CAP, tokens, half), BF),
            pltpu.VMEM((rows, feats, block), BF),
            pltpu.VMEM((8, 128), jnp.int32),
            pltpu.VMEM((rows, 128), jnp.int32),
            pltpu.VMEM((rows, 128), jnp.int32),
            pltpu.VMEM((rows, 8, 128), jnp.int32),
            pltpu.SMEM((rows, 128), jnp.int32),
            pltpu.SMEM((8, 128), jnp.int32),
            dma((2,)),
            dma((2,)),
            pltpu.SemaphoreType.REGULAR,
            dma((2,)),
            dma((rows,)),
            dma((rows,)),
            dma((rows,)),
            dma((rows,)),
            dma((rows,)),
            dma((rows,)),
            dma((heads,)),
            dma((carriers,)),
            dma((heads,)),
            dma((carriers,)),
            dma((carriers,)),
            dma((carriers,)),
            dma((carriers,)),
            dma((carriers,)),
            dma((2,)),
            dma((2,)),
        ],
        compiler_params=pltpu.CompilerParams(
            collective_id=0, has_side_effects=True, vmem_limit_bytes=16 << 20
        ),
        name="exchange",
    )(block_list, block_slot, pool_latent, pool_rope, new_latent, new_rope)
    total = (blocks * block) + 2 * queries
    return pl.pallas_call(
        functools.partial(attend, 1.0 / math.sqrt(NOPE + ROPE)),
        out_shape=shape(q_nope.shape, BF),
        in_specs=[smem] + [vmem] * 12,
        out_specs=vmem,
        scratch_shapes=[
            pltpu.VMEM((total, 2 * half), BF),
            pltpu.VMEM((total, 2 * ROPE), BF),
            pltpu.VMEM((total, 2 * ROPE), BF),
            pltpu.VMEM((queries, total), F32),
        ],
        compiler_params=pltpu.CompilerParams(vmem_limit_bytes=32 << 20),
        name="attend",
    )(
        prefix_len,
        q_nope,
        q_rope,
        lat_mine,
        lat_other,
        rope_mine,
        rope_other,
        new_latent,
        new_lat_other,
        new_rope,
        new_rope_other,
        w_uk,
        w_uv,
    )


def solution(mesh):
    placed = (
        P(("groups", "req", "sub"), "head"),
        P(("groups", "req", "sub"), "head"),
        P(("groups", "req", "sub"), None),
        P(("groups", "req", "sub"), None),
        P(("groups", "req"), None, "sub"),
        P(("groups", "req"), None, None),
        P(None, "head"),
        P(None, "head"),
        P(("groups", "req"), None),
        P(("groups", "req")),
        P("groups"),
    )
    return jax.shard_map(
        shards,
        mesh=mesh,
        in_specs=placed,
        out_specs=P(("groups", "req", "sub"), "head"),
        check_vma=False,
    )
```

```python
import functools
import math

import jax
import jax.numpy as jnp
from jax import lax
from jax.experimental import pallas as pl
from jax.experimental.pallas import tpu as pltpu
from jax.sharding import PartitionSpec as P

NOPE = 128
ROPE = 64
VDIM = 128
CAP = 2
MESH = pl.DeviceIdType.MESH
BF = jnp.bfloat16
F32 = jnp.float32


def exchange(
    blocks,
    pool_local,
    scale,
    list_hbm,
    slot_hbm,
    pool_lat,
    pool_rope,
    new_lat,
    new_rope,
    length_ref,
    q_nope,
    q_rope,
    w_uk,
    w_uv,
    out,
    lat_mine,
    lat_other,
    rope_mine,
    rope_other,
    new_lat_other,
    new_rope_other,
    new_lat_v,
    new_rope_v,
    keys,
    rope_even,
    rope_odd,
    bias,
    q_nope_v,
    q_rope_v,
    w_uk_v,
    w_uv_v,
    load_sem,
    pool_l,
    pool_r,
    send_l,
    send_r,
    got_l,
    got_r,
    own_v,
    table_in,
    table_out,
    asked_v,
    table_s,
    asked_s,
    list_ref,
    slot_ref,
    pool_sem,
    small_sem,
    hello_sem,
    table_sem,
    ask_send,
    ask_recv,
    lat_send,
    lat_recv,
    rope_send,
    rope_recv,
    xlat_send,
    xlat_recv,
    xrope_send,
    xrope_recv,
    slat_send,
    slat_recv,
    srope_send,
    srope_recv,
    snew_send,
    snew_recv,
):
    rows = lax.axis_size("req")
    heads = lax.axis_size("head")
    row = lax.axis_index("req")
    lane = lax.axis_index("head")
    core = lax.axis_index("sub")
    other = {"sub": 1 - core}
    carriers = heads
    tokens = pool_l.shape[1]
    feats = pool_r.shape[1]
    part = lane
    turn = jnp.where(lane == 0, 1, 0)
    place = lax.rem(row + rows - turn, rows)

    def at(p):
        return lax.rem(p + turn, rows)

    token_at = pl.multiple_of(part * tokens, tokens)
    feat_at = pl.multiple_of(part * feats, feats)
    barrier = pltpu.get_barrier_semaphore()

    for step in range(1, heads):
        pl.semaphore_signal(
            barrier, inc=1, device_id={"head": lax.rem(lane + step, heads)}, device_id_type=MESH
        )
    pl.semaphore_signal(barrier, inc=1, device_id=other, device_id_type=MESH)

    def tell(p, carry):
        pl.semaphore_signal(barrier, inc=1, device_id={"req": at(p)}, device_id_type=MESH)
        return carry

    lax.fori_loop(place + 1, rows, tell, 0)

    load_l = pltpu.make_async_copy(
        pool_lat.at[:, pl.ds(token_at, tokens), :], pool_l, pool_sem.at[0]
    )
    load_r = pltpu.make_async_copy(
        pool_rope.at[:, pl.ds(feat_at, feats), :], pool_r, pool_sem.at[1]
    )

    load_l.start()
    load_r.start()
    loads = [
        pltpu.make_async_copy(src, dst, load_sem.at[i])
        for i, (src, dst) in enumerate(
            (
                (new_lat, new_lat_v),
                (new_rope, new_rope_v),
                (w_uk, w_uk_v),
                (q_nope, q_nope_v),
                (q_rope, q_rope_v),
                (w_uv, w_uv_v),
            )
        )
    ]
    for load in loads:
        load.start()

    to_list = pltpu.make_async_copy(list_hbm, list_ref, small_sem.at[0])
    to_slot = pltpu.make_async_copy(slot_hbm, slot_ref, small_sem.at[1])
    to_list.start()
    to_slot.start()
    to_list.wait()
    to_slot.wait()
    physical = [slot_ref[list_ref[0, j]] for j in range(blocks)]
    column = lax.broadcasted_iota(jnp.int32, own_v.shape, 1)
    own = jnp.zeros(own_v.shape, jnp.int32)
    for j in range(blocks):
        own = jnp.where(column == j, physical[j], own)
    own_v[...] = own

    @pl.when(place > 0)
    def _():
        pl.semaphore_wait(barrier, heads + place)

    def lat_copy(p, sem_at):
        return pltpu.make_async_remote_copy(
            send_l.at[p], got_l.at[row], lat_send.at[p], lat_recv.at[sem_at], {"req": p}, MESH
        )

    def rope_copy(p, sem_at):
        return pltpu.make_async_remote_copy(
            send_r.at[p], got_r.at[row], rope_send.at[p], rope_recv.at[sem_at], {"req": p}, MESH
        )

    def ask_copy(p):
        return pltpu.make_async_remote_copy(
            own_v, asked_v.at[row], ask_send.at[p], ask_recv.at[row], {"req": p}, MESH
        )

    def chosen(read):
        count = jnp.int32(0)
        first = jnp.int32(0)
        second = jnp.int32(0)
        for j in range(blocks):
            where = read(j)
            local = where - row * pool_local
            here = (local >= 0) & (local < pool_local)
            first = jnp.where(here & (count == 0), local, first)
            second = jnp.where(here & (count == 1), local, second)
            count = count + here.astype(jnp.int32)
        return first, second

    def serve(p, read):
        first, second = chosen(read)
        send_l[p, 0] = pool_l[first]
        send_l[p, 1] = pool_l[second]
        send_r[p] = pool_r[jnp.where(core == 0, first, second)]
        lat_copy(p, row).start()
        rope_copy(p, row).start()

    table_copy = pltpu.make_async_remote_copy(
        table_out, table_in, table_sem.at[0], table_sem.at[1], {"req": lax.rem(row + 1, rows)}, MESH
    )

    @pl.when(place > 0)
    def _():
        pl.semaphore_signal(
            hello_sem, inc=1, device_id={"req": at(place - 1)}, device_id_type=MESH
        )

    def ask(p, carry):
        ask_copy(at(p)).start()
        return carry

    lax.fori_loop(0, place, ask, 0)
    load_l.wait()
    load_r.wait()

    @pl.when(place > 0)
    def _():
        table_copy.wait_recv()

    line = lax.broadcasted_iota(jnp.int32, table_out.shape, 0)
    mine = jnp.broadcast_to(own_v[0:1, :], table_out.shape)
    below_me = lax.rem(line + rows - turn, rows) < place
    known = jnp.where(below_me, table_in[...], 0)
    table_out[...] = jnp.where(line == row, mine, known)

    @pl.when(place < rows - 1)
    def _():
        pl.semaphore_wait(hello_sem, 1)
        table_copy.start()

    @pl.when(place > 0)
    def _():
        to_s = pltpu.make_async_copy(table_in, table_s, small_sem.at[0])
        to_s.start()
        to_s.wait()

        def below(p, carry):
            r = at(p)
            serve(r, lambda j: table_s[r, j])
            return carry

        lax.fori_loop(0, place, below, 0)

    @pl.when(place < rows - 1)
    def _():

        def above(p, carry):
            r = at(p)
            pltpu.make_async_remote_copy(
                own_v, asked_v.at[r], ask_send.at[r], ask_recv.at[r], {"req": r}, MESH
            ).wait_recv()
            to_s = pltpu.make_async_copy(asked_v.at[r], asked_s, small_sem.at[1])
            to_s.start()
            to_s.wait()
            serve(r, lambda j: asked_s[0, j])
            return carry

        lax.fori_loop(place + 1, rows, above, 0)

    first, second = chosen(lambda j: physical[j])
    got_l[row, 0] = pool_l[first]
    got_l[row, 1] = pool_l[second]
    got_r[row] = pool_r[jnp.where(core == 0, first, second)]

    def arrived(p, carry):
        @pl.when(p != row)
        def _():
            lat_copy(p, p).wait_recv()
            rope_copy(p, p).wait_recv()

        return carry

    lax.fori_loop(0, rows, arrived, 0)

    for j in range(blocks):
        owner = physical[j] // pool_local
        rank = jnp.int32(0)
        for i in range(j):
            rank = rank + (physical[i] // pool_local == owner).astype(jnp.int32)
        lat_mine[j, pl.ds(token_at, tokens), :] = got_l[owner, jnp.minimum(rank, CAP - 1)]
        piece = got_r[owner]
        rope_mine[j, pl.ds(feat_at, feats), :] = jnp.where(
            rank == core, piece, jnp.zeros_like(piece)
        )

    @pl.when(place == 0)
    def _():
        pl.semaphore_wait(barrier, heads)

    for load in loads:
        load.wait()
    new_copies = [
        pltpu.make_async_remote_copy(
            src, dst, snew_send.at[i], snew_recv.at[i], other, MESH
        )
        for i, (src, dst) in enumerate(((new_lat_v, new_lat_other), (new_rope_v, new_rope_other)))
    ]
    for copy in new_copies:
        copy.start()

    def lat_piece(k):
        return pl.ds(pl.multiple_of(k * tokens, tokens), tokens)

    def rope_piece(k):
        return pl.ds(pl.multiple_of(k * feats, feats), feats)

    def xlat_copy(k, peer):
        at = lat_piece(k)
        return pltpu.make_async_remote_copy(
            lat_mine.at[:, at, :],
            lat_mine.at[:, at, :],
            xlat_send.at[peer],
            xlat_recv.at[k],
            {"head": peer},
            MESH,
        )

    def xrope_copy(k, peer):
        at = rope_piece(k)
        return pltpu.make_async_remote_copy(
            rope_mine.at[:, at, :],
            rope_mine.at[:, at, :],
            xrope_send.at[peer],
            xrope_recv.at[k],
            {"head": peer},
            MESH,
        )

    def sub_copies(k):
        at, fat = lat_piece(k), rope_piece(k)
        return (
            pltpu.make_async_remote_copy(
                lat_mine.at[:, at, :],
                lat_other.at[:, at, :],
                slat_send.at[k],
                slat_recv.at[k],
                other,
                MESH,
            ),
            pltpu.make_async_remote_copy(
                rope_mine.at[:, fat, :],
                rope_other.at[:, fat, :],
                srope_send.at[k],
                srope_recv.at[k],
                other,
                MESH,
            ),
        )

    order = [0]
    for step in range(heads // 2, 0, -1):
        for peer in (step, heads - step):
            if peer not in order:
                order.append(peer)
    order = order[1:]

    for step in order:
        peer = lax.rem(lane + step, heads)
        xlat_copy(part, peer).start()
        xrope_copy(part, peer).start()
    for copy in sub_copies(part):
        copy.start()

    for k in range(carriers):

        @pl.when(part != k)
        def _(k=k):
            xlat_copy(k, lane).wait_recv()
            xrope_copy(k, lane).wait_recv()
            for copy in sub_copies(k):
                copy.start()

    for k in range(carriers):
        for copy in sub_copies(k):
            copy.wait()
    for copy in new_copies:
        copy.wait()

    blocks, block, half = lat_mine.shape
    prefix = blocks * block
    queries = q_nope.shape[0]
    total = keys.shape[0]
    here = pl.ds(pl.multiple_of(core * half, half), half)
    there = pl.ds(pl.multiple_of((1 - core) * half, half), half)
    for j in range(blocks):
        keys[pl.ds(j * block, block), here] = lat_mine[j]
        keys[pl.ds(j * block, block), there] = lat_other[j]
    keys[pl.ds(prefix, queries), :] = new_lat_v[...]
    keys[pl.ds(prefix + queries, queries), :] = new_lat_other[...]

    def put_rope(at, piece):
        turned = piece.astype(F32).T.astype(BF)
        blank = jnp.zeros_like(turned)
        rope_even[pl.ds(at, turned.shape[0]), :] = jnp.concatenate([turned, blank], axis=1)
        rope_odd[pl.ds(at, turned.shape[0]), :] = jnp.concatenate([blank, turned], axis=1)

    for j in range(blocks):
        put_rope(j * block, rope_mine[j] + rope_other[j])
    put_rope(prefix, new_rope_v[...])
    put_rope(prefix + queries, new_rope_other[...])

    key = lax.broadcasted_iota(jnp.int32, (queries, total), 1)
    query = lax.broadcasted_iota(jnp.int32, (queries, total), 0)
    last = jnp.where(core == 1, total, prefix + queries)
    hidden = F32(-1e30)
    in_prefix = jnp.where(key < length_ref[0], F32(0.0), hidden)
    in_mine = jnp.where(key - prefix <= query, F32(0.0), hidden)
    in_other = jnp.where(key < last, F32(0.0), hidden)
    fresh = jnp.where(key < prefix + queries, in_mine, in_other)
    bias[...] = jnp.where(key < prefix, in_prefix, fresh)

    def pair(i, carry):
        cols = pl.ds(pl.multiple_of(i * 2 * NOPE, 2 * NOPE), 2 * NOPE)
        k2 = jnp.dot(keys[...], w_uk_v[:, cols], preferred_element_type=F32).astype(BF)
        v2 = jnp.dot(keys[...], w_uv_v[:, cols], preferred_element_type=F32).astype(BF)
        qr = q_rope_v[:, pl.ds(pl.multiple_of(i * 2 * ROPE, 2 * ROPE), 2 * ROPE)]
        qn = q_nope_v[:, cols]
        outs = []
        for e, kr in ((0, rope_even), (1, rope_odd)):
            kcat = jnp.concatenate([k2[:, e * NOPE : (e + 1) * NOPE], kr[...]], axis=1)
            qcat = jnp.concatenate([qn[:, e * NOPE : (e + 1) * NOPE], qr], axis=1)
            s = lax.dot_general(
                qcat, kcat, (((1,), (1,)), ((), ())), preferred_element_type=F32
            )
            s = s * scale + bias[...]
            peak = jnp.max(s, axis=1, keepdims=True)
            expo = jnp.exp(s - peak)
            weights = (expo * (1.0 / jnp.sum(expo, axis=1, keepdims=True))).astype(BF)
            outs.append(
                jnp.dot(
                    weights, v2[:, e * VDIM : (e + 1) * VDIM], preferred_element_type=F32
                ).astype(BF)
            )
        out[:, cols] = jnp.concatenate(outs, axis=1)
        return carry

    lax.fori_loop(0, q_nope.shape[1] // (2 * NOPE), pair, 0)

    for step in order:
        peer = lax.rem(lane + step, heads)
        xlat_copy(part, peer).wait_send()
        xrope_copy(part, peer).wait_send()

    def sent(p, carry):
        r = at(p)

        @pl.when(p != place)
        def _():
            lat_copy(r, row).wait_send()
            rope_copy(r, row).wait_send()

        @pl.when(p < place)
        def _():
            ask_copy(r).wait_send()

        return carry

    lax.fori_loop(0, rows, sent, 0)

    @pl.when(place < rows - 1)
    def _():
        table_copy.wait_send()


def shards(
    q_nope,
    q_rope,
    new_latent,
    new_rope,
    pool_latent,
    pool_rope,
    w_uk,
    w_uv,
    block_list,
    prefix_len,
    block_slot,
):
    rows = lax.axis_size("req")
    heads = lax.axis_size("head")
    pool_local, block, half = pool_latent.shape
    blocks = block_list.shape[1]
    queries = q_nope.shape[0]
    carriers = heads
    tokens = block // carriers
    feats = ROPE // carriers
    pool_rope = jnp.swapaxes(pool_rope, 1, 2)
    new_rope = new_rope.T
    vmem = pl.BlockSpec(memory_space=pltpu.VMEM)
    smem = pl.BlockSpec(memory_space=pltpu.SMEM)
    hbm = pl.BlockSpec(memory_space=pltpu.HBM)
    dma = pltpu.SemaphoreType.DMA
    shape = jax.ShapeDtypeStruct
    total = (blocks * block) + 2 * queries
    return pl.pallas_call(
        functools.partial(exchange, blocks, pool_local, 1.0 / math.sqrt(NOPE + ROPE)),
        out_shape=shape(q_nope.shape, BF),
        in_specs=[hbm] * 6 + [smem] + [hbm] * 4,
        out_specs=vmem,
        scratch_shapes=[
            pltpu.VMEM((blocks, block, half), BF),
            pltpu.VMEM((blocks, block, half), BF),
            pltpu.VMEM((blocks, ROPE, block), BF),
            pltpu.VMEM((blocks, ROPE, block), BF),
            pltpu.VMEM(new_latent.shape, BF),
            pltpu.VMEM(new_rope.shape, BF),
            pltpu.VMEM(new_latent.shape, BF),
            pltpu.VMEM(new_rope.shape, BF),
            pltpu.VMEM((total, 2 * half), BF),
            pltpu.VMEM((total, 2 * ROPE), BF),
            pltpu.VMEM((total, 2 * ROPE), BF),
            pltpu.VMEM((queries, total), F32),
            pltpu.VMEM(q_nope.shape, BF),
            pltpu.VMEM(q_rope.shape, BF),
            pltpu.VMEM(w_uk.shape, BF),
            pltpu.VMEM(w_uv.shape, BF),
            dma((6,)),
            pltpu.VMEM((pool_local, tokens, half), BF),
            pltpu.VMEM((pool_local, feats, block), BF),
            pltpu.VMEM((rows, CAP, tokens, half), BF),
            pltpu.VMEM((rows, feats, block), BF),
            pltpu.VMEM((rows, CAP, tokens, half), BF),
            pltpu.VMEM((rows, feats, block), BF),
            pltpu.VMEM((8, 128), jnp.int32),
            pltpu.VMEM((rows, 128), jnp.int32),
            pltpu.VMEM((rows, 128), jnp.int32),
            pltpu.VMEM((rows, 8, 128), jnp.int32),
            pltpu.SMEM((rows, 128), jnp.int32),
            pltpu.SMEM((8, 128), jnp.int32),
            pltpu.SMEM(block_list.shape, jnp.int32),
            pltpu.SMEM(block_slot.shape, jnp.int32),
            dma((2,)),
            dma((2,)),
            pltpu.SemaphoreType.REGULAR,
            dma((2,)),
            dma((rows,)),
            dma((rows,)),
            dma((rows,)),
            dma((rows,)),
            dma((rows,)),
            dma((rows,)),
            dma((heads,)),
            dma((carriers,)),
            dma((heads,)),
            dma((carriers,)),
            dma((carriers,)),
            dma((carriers,)),
            dma((carriers,)),
            dma((carriers,)),
            dma((2,)),
            dma((2,)),
        ],
        compiler_params=pltpu.CompilerParams(
            collective_id=0, has_side_effects=True, vmem_limit_bytes=62 << 20
        ),
        name="fused",
    )(
        block_list,
        block_slot,
        pool_latent,
        pool_rope,
        new_latent,
        new_rope,
        prefix_len,
        q_nope,
        q_rope,
        w_uk,
        w_uv,
    )


def solution(mesh):
    placed = (
        P(("groups", "req", "sub"), "head"),
        P(("groups", "req", "sub"), "head"),
        P(("groups", "req", "sub"), None),
        P(("groups", "req", "sub"), None),
        P(("groups", "req"), None, "sub"),
        P(("groups", "req"), None, None),
        P(None, "head"),
        P(None, "head"),
        P(("groups", "req"), None),
        P(("groups", "req")),
        P("groups"),
    )
    return jax.shard_map(
        shards,
        mesh=mesh,
        in_specs=placed,
        out_specs=P(("groups", "req", "sub"), "head"),
        check_vma=False,
    )
```

```python
import functools
import math

import jax
import jax.numpy as jnp
from jax import lax
from jax.experimental import pallas as pl
from jax.experimental.pallas import tpu as pltpu
from jax.sharding import PartitionSpec as P

NOPE = 128
ROPE = 64
VDIM = 128
CAP = 2
EARLY = 4
MESH = pl.DeviceIdType.MESH
BF = jnp.bfloat16
F32 = jnp.float32


def exchange(
    blocks,
    pool_local,
    scale,
    list_hbm,
    slot_hbm,
    pool_lat,
    pool_rope,
    new_lat,
    new_rope,
    length_ref,
    q_nope,
    q_rope,
    w_uk,
    w_uv,
    out,
    lat_mine,
    lat_other,
    rope_mine,
    rope_other,
    new_lat_other,
    new_rope_other,
    new_lat_v,
    new_rope_v,
    keys,
    rope_even,
    rope_odd,
    bias,
    q_nope_v,
    q_rope_v,
    w_uk_v,
    w_uv_v,
    load_sem,
    pool_l,
    pool_r,
    send_l,
    send_r,
    got_l,
    got_r,
    own_v,
    near_v,
    table_in,
    table_out,
    asked_v,
    table_s,
    asked_s,
    list_ref,
    slot_ref,
    pool_sem,
    small_sem,
    hello_sem,
    near_sem,
    table_sem,
    ask_send,
    ask_recv,
    lat_send,
    lat_recv,
    rope_send,
    rope_recv,
    xlat_send,
    xlat_recv,
    xrope_send,
    xrope_recv,
    slat_send,
    slat_recv,
    srope_send,
    srope_recv,
    snew_send,
    snew_recv,
):
    rows = lax.axis_size("req")
    heads = lax.axis_size("head")
    row = lax.axis_index("req")
    lane = lax.axis_index("head")
    core = lax.axis_index("sub")
    other = {"sub": 1 - core}
    carriers = heads
    tokens = pool_l.shape[1]
    feats = pool_r.shape[1]
    part = lane
    turn = jnp.where((lane == 0) & (core == 0), 1, 0)
    place = lax.rem(row + rows - turn, rows)

    def at(p):
        return lax.rem(p + turn, rows)

    token_at = pl.multiple_of(part * tokens, tokens)
    feat_at = pl.multiple_of(part * feats, feats)
    barrier = pltpu.get_barrier_semaphore()

    for step in range(1, heads):
        pl.semaphore_signal(
            barrier, inc=1, device_id={"head": lax.rem(lane + step, heads)}, device_id_type=MESH
        )
    pl.semaphore_signal(barrier, inc=1, device_id=other, device_id_type=MESH)

    def tell(p, carry):
        pl.semaphore_signal(barrier, inc=1, device_id={"req": at(p)}, device_id_type=MESH)
        return carry

    lax.fori_loop(place + 1, rows, tell, 0)

    load_l = pltpu.make_async_copy(
        pool_lat.at[:, pl.ds(token_at, tokens), :], pool_l, pool_sem.at[0]
    )
    load_r = pltpu.make_async_copy(
        pool_rope.at[:, pl.ds(feat_at, feats), :], pool_r, pool_sem.at[1]
    )

    load_l.start()
    load_r.start()
    loads = [
        pltpu.make_async_copy(src, dst, load_sem.at[i])
        for i, (src, dst) in enumerate(
            (
                (new_lat, new_lat_v),
                (new_rope, new_rope_v),
                (w_uk, w_uk_v),
                (q_nope, q_nope_v),
                (q_rope, q_rope_v),
                (w_uv, w_uv_v),
            )
        )
    ]
    for load in loads:
        load.start()

    to_list = pltpu.make_async_copy(list_hbm, list_ref, small_sem.at[0])
    to_slot = pltpu.make_async_copy(slot_hbm, slot_ref, small_sem.at[1])
    to_list.start()
    to_slot.start()
    to_list.wait()
    to_slot.wait()
    physical = [slot_ref[list_ref[0, j]] for j in range(blocks)]
    column = lax.broadcasted_iota(jnp.int32, own_v.shape, 1)
    own = jnp.zeros(own_v.shape, jnp.int32)
    for j in range(blocks):
        own = jnp.where(column == j, physical[j], own)
    own_v[...] = own

    @pl.when(place > 0)
    def _():
        pl.semaphore_wait(barrier, heads + place)

    def lat_copy(p, sem_at):
        return pltpu.make_async_remote_copy(
            send_l.at[p], got_l.at[row], lat_send.at[p], lat_recv.at[sem_at], {"req": p}, MESH
        )

    def rope_copy(p, sem_at):
        return pltpu.make_async_remote_copy(
            send_r.at[p], got_r.at[row], rope_send.at[p], rope_recv.at[sem_at], {"req": p}, MESH
        )

    def ask_copy(p):
        return pltpu.make_async_remote_copy(
            own_v, asked_v.at[row], ask_send.at[p], ask_recv.at[row], {"req": p}, MESH
        )

    def chosen(read):
        count = jnp.int32(0)
        first = jnp.int32(0)
        second = jnp.int32(0)
        for j in range(blocks):
            where = read(j)
            local = where - row * pool_local
            here = (local >= 0) & (local < pool_local)
            first = jnp.where(here & (count == 0), local, first)
            second = jnp.where(here & (count == 1), local, second)
            count = count + here.astype(jnp.int32)
        return first, second

    def serve(p, read):
        first, second = chosen(read)
        send_l[p, 0] = pool_l[first]
        send_l[p, 1] = pool_l[second]
        send_r[p] = pool_r[jnp.where(core == 0, first, second)]
        lat_copy(p, row).start()
        rope_copy(p, row).start()

    table_copy = pltpu.make_async_remote_copy(
        table_out,
        table_in,
        table_sem.at[0],
        table_sem.at[1],
        {"req": at(lax.rem(place + 2, rows))},
        MESH,
    )
    near_copy = pltpu.make_async_remote_copy(
        own_v, near_v, near_sem.at[0], near_sem.at[1], {"req": at(lax.rem(place + 1, rows))}, MESH
    )

    for step in (1, 2):

        @pl.when(place >= step)
        def _(step=step):
            pl.semaphore_signal(
                hello_sem.at[step - 1],
                inc=1,
                device_id={"req": at(place - step)},
                device_id_type=MESH,
            )

    def ask(p, carry):
        ask_copy(at(p)).start()
        return carry

    lax.fori_loop(0, place, ask, 0)
    load_l.wait()
    load_r.wait()

    @pl.when(place < rows - 1)
    def _():
        pl.semaphore_wait(hello_sem.at[0], 1)
        near_copy.start()

    @pl.when(place > 1)
    def _():
        table_copy.wait_recv()

    @pl.when(place > 0)
    def _():
        near_copy.wait_recv()

    line = lax.broadcasted_iota(jnp.int32, table_out.shape, 0)
    line_place = lax.rem(line + rows - turn, rows)
    mine = jnp.broadcast_to(own_v[0:1, :], table_out.shape)
    near = jnp.broadcast_to(near_v[0:1, :], table_out.shape)
    known = jnp.where(line_place < place - 1, table_in[...], 0)
    known = jnp.where(line_place == place - 1, near, known)
    table_out[...] = jnp.where(line == row, mine, known)

    def below(p, carry):
        r = at(p)
        serve(r, lambda j: table_s[r, j])
        return carry

    early = jnp.minimum(place, EARLY)

    @pl.when(place > 0)
    def _():
        to_s = pltpu.make_async_copy(table_out, table_s, small_sem.at[0])
        to_s.start()
        to_s.wait()
        lax.fori_loop(0, early, below, 0)

    @pl.when(place < rows - 2)
    def _():
        pl.semaphore_wait(hello_sem.at[1], 1)
        table_copy.start()

    lax.fori_loop(early, place, below, 0)

    @pl.when(place < rows - 1)
    def _():

        def above(p, carry):
            r = at(p)
            pltpu.make_async_remote_copy(
                own_v, asked_v.at[r], ask_send.at[r], ask_recv.at[r], {"req": r}, MESH
            ).wait_recv()
            to_s = pltpu.make_async_copy(asked_v.at[r], asked_s, small_sem.at[1])
            to_s.start()
            to_s.wait()
            serve(r, lambda j: asked_s[0, j])
            return carry

        lax.fori_loop(place + 1, rows, above, 0)

    first, second = chosen(lambda j: physical[j])
    got_l[row, 0] = pool_l[first]
    got_l[row, 1] = pool_l[second]
    got_r[row] = pool_r[jnp.where(core == 0, first, second)]

    def arrived(p, carry):
        @pl.when(p != row)
        def _():
            lat_copy(p, p).wait_recv()
            rope_copy(p, p).wait_recv()

        return carry

    lax.fori_loop(0, rows, arrived, 0)

    for j in range(blocks):
        owner = physical[j] // pool_local
        rank = jnp.int32(0)
        for i in range(j):
            rank = rank + (physical[i] // pool_local == owner).astype(jnp.int32)
        lat_mine[j, pl.ds(token_at, tokens), :] = got_l[owner, jnp.minimum(rank, CAP - 1)]
        piece = got_r[owner]
        rope_mine[j, pl.ds(feat_at, feats), :] = jnp.where(
            rank == core, piece, jnp.zeros_like(piece)
        )

    @pl.when(place == 0)
    def _():
        pl.semaphore_wait(barrier, heads)

    for load in loads:
        load.wait()
    new_copies = [
        pltpu.make_async_remote_copy(
            src, dst, snew_send.at[i], snew_recv.at[i], other, MESH
        )
        for i, (src, dst) in enumerate(((new_lat_v, new_lat_other), (new_rope_v, new_rope_other)))
    ]
    for copy in new_copies:
        copy.start()

    def lat_piece(k):
        return pl.ds(pl.multiple_of(k * tokens, tokens), tokens)

    def rope_piece(k):
        return pl.ds(pl.multiple_of(k * feats, feats), feats)

    def xlat_copy(k, peer):
        at = lat_piece(k)
        return pltpu.make_async_remote_copy(
            lat_mine.at[:, at, :],
            lat_mine.at[:, at, :],
            xlat_send.at[peer],
            xlat_recv.at[k],
            {"head": peer},
            MESH,
        )

    def xrope_copy(k, peer):
        at = rope_piece(k)
        return pltpu.make_async_remote_copy(
            rope_mine.at[:, at, :],
            rope_mine.at[:, at, :],
            xrope_send.at[peer],
            xrope_recv.at[k],
            {"head": peer},
            MESH,
        )

    def sub_copies(k):
        at, fat = lat_piece(k), rope_piece(k)
        return (
            pltpu.make_async_remote_copy(
                lat_mine.at[:, at, :],
                lat_other.at[:, at, :],
                slat_send.at[k],
                slat_recv.at[k],
                other,
                MESH,
            ),
            pltpu.make_async_remote_copy(
                rope_mine.at[:, fat, :],
                rope_other.at[:, fat, :],
                srope_send.at[k],
                srope_recv.at[k],
                other,
                MESH,
            ),
        )

    order = [0]
    for step in range(heads // 2, 0, -1):
        for peer in (step, heads - step):
            if peer not in order:
                order.append(peer)
    order = order[1:]

    for step in order:
        peer = lax.rem(lane + step, heads)
        xlat_copy(part, peer).start()
        xrope_copy(part, peer).start()
    for copy in sub_copies(part):
        copy.start()

    for k in range(carriers):

        @pl.when(part != k)
        def _(k=k):
            xlat_copy(k, lane).wait_recv()
            xrope_copy(k, lane).wait_recv()
            for copy in sub_copies(k):
                copy.start()

    for k in range(carriers):
        for copy in sub_copies(k):
            copy.wait()
    for copy in new_copies:
        copy.wait()

    blocks, block, half = lat_mine.shape
    prefix = blocks * block
    queries = q_nope.shape[0]
    total = keys.shape[0]
    here = pl.ds(pl.multiple_of(core * half, half), half)
    there = pl.ds(pl.multiple_of((1 - core) * half, half), half)
    for j in range(blocks):
        keys[pl.ds(j * block, block), here] = lat_mine[j]
        keys[pl.ds(j * block, block), there] = lat_other[j]
    keys[pl.ds(prefix, queries), :] = new_lat_v[...]
    keys[pl.ds(prefix + queries, queries), :] = new_lat_other[...]

    def put_rope(at, piece):
        turned = piece.astype(F32).T.astype(BF)
        blank = jnp.zeros_like(turned)
        rope_even[pl.ds(at, turned.shape[0]), :] = jnp.concatenate([turned, blank], axis=1)
        rope_odd[pl.ds(at, turned.shape[0]), :] = jnp.concatenate([blank, turned], axis=1)

    for j in range(blocks):
        put_rope(j * block, rope_mine[j] + rope_other[j])
    put_rope(prefix, new_rope_v[...])
    put_rope(prefix + queries, new_rope_other[...])

    key = lax.broadcasted_iota(jnp.int32, (queries, total), 1)
    query = lax.broadcasted_iota(jnp.int32, (queries, total), 0)
    last = jnp.where(core == 1, total, prefix + queries)
    hidden = F32(-1e30)
    in_prefix = jnp.where(key < length_ref[0], F32(0.0), hidden)
    in_mine = jnp.where(key - prefix <= query, F32(0.0), hidden)
    in_other = jnp.where(key < last, F32(0.0), hidden)
    fresh = jnp.where(key < prefix + queries, in_mine, in_other)
    bias[...] = jnp.where(key < prefix, in_prefix, fresh)

    def pair(i, carry):
        cols = pl.ds(pl.multiple_of(i * 2 * NOPE, 2 * NOPE), 2 * NOPE)
        k2 = jnp.dot(keys[...], w_uk_v[:, cols], preferred_element_type=F32).astype(BF)
        v2 = jnp.dot(keys[...], w_uv_v[:, cols], preferred_element_type=F32).astype(BF)
        qr = q_rope_v[:, pl.ds(pl.multiple_of(i * 2 * ROPE, 2 * ROPE), 2 * ROPE)]
        qn = q_nope_v[:, cols]
        outs = []
        for e, kr in ((0, rope_even), (1, rope_odd)):
            kcat = jnp.concatenate([k2[:, e * NOPE : (e + 1) * NOPE], kr[...]], axis=1)
            qcat = jnp.concatenate([qn[:, e * NOPE : (e + 1) * NOPE], qr], axis=1)
            s = lax.dot_general(
                qcat, kcat, (((1,), (1,)), ((), ())), preferred_element_type=F32
            )
            s = s * scale + bias[...]
            peak = jnp.max(s, axis=1, keepdims=True)
            expo = jnp.exp(s - peak)
            weights = (expo * (1.0 / jnp.sum(expo, axis=1, keepdims=True))).astype(BF)
            outs.append(
                jnp.dot(
                    weights, v2[:, e * VDIM : (e + 1) * VDIM], preferred_element_type=F32
                ).astype(BF)
            )
        out[:, cols] = jnp.concatenate(outs, axis=1)
        return carry

    lax.fori_loop(0, q_nope.shape[1] // (2 * NOPE), pair, 0)

    for step in order:
        peer = lax.rem(lane + step, heads)
        xlat_copy(part, peer).wait_send()
        xrope_copy(part, peer).wait_send()

    def sent(p, carry):
        r = at(p)

        @pl.when(p != place)
        def _():
            lat_copy(r, row).wait_send()
            rope_copy(r, row).wait_send()

        @pl.when(p < place)
        def _():
            ask_copy(r).wait_send()

        return carry

    lax.fori_loop(0, rows, sent, 0)

    @pl.when(place < rows - 1)
    def _():
        near_copy.wait_send()

    @pl.when(place < rows - 2)
    def _():
        table_copy.wait_send()


def shards(
    q_nope,
    q_rope,
    new_latent,
    new_rope,
    pool_latent,
    pool_rope,
    w_uk,
    w_uv,
    block_list,
    prefix_len,
    block_slot,
):
    rows = lax.axis_size("req")
    heads = lax.axis_size("head")
    pool_local, block, half = pool_latent.shape
    blocks = block_list.shape[1]
    queries = q_nope.shape[0]
    carriers = heads
    tokens = block // carriers
    feats = ROPE // carriers
    pool_rope = jnp.swapaxes(pool_rope, 1, 2)
    new_rope = new_rope.T
    vmem = pl.BlockSpec(memory_space=pltpu.VMEM)
    smem = pl.BlockSpec(memory_space=pltpu.SMEM)
    hbm = pl.BlockSpec(memory_space=pltpu.HBM)
    dma = pltpu.SemaphoreType.DMA
    shape = jax.ShapeDtypeStruct
    total = (blocks * block) + 2 * queries
    return pl.pallas_call(
        functools.partial(exchange, blocks, pool_local, 1.0 / math.sqrt(NOPE + ROPE)),
        out_shape=shape(q_nope.shape, BF),
        in_specs=[hbm] * 6 + [smem] + [hbm] * 4,
        out_specs=vmem,
        scratch_shapes=[
            pltpu.VMEM((blocks, block, half), BF),
            pltpu.VMEM((blocks, block, half), BF),
            pltpu.VMEM((blocks, ROPE, block), BF),
            pltpu.VMEM((blocks, ROPE, block), BF),
            pltpu.VMEM(new_latent.shape, BF),
            pltpu.VMEM(new_rope.shape, BF),
            pltpu.VMEM(new_latent.shape, BF),
            pltpu.VMEM(new_rope.shape, BF),
            pltpu.VMEM((total, 2 * half), BF),
            pltpu.VMEM((total, 2 * ROPE), BF),
            pltpu.VMEM((total, 2 * ROPE), BF),
            pltpu.VMEM((queries, total), F32),
            pltpu.VMEM(q_nope.shape, BF),
            pltpu.VMEM(q_rope.shape, BF),
            pltpu.VMEM(w_uk.shape, BF),
            pltpu.VMEM(w_uv.shape, BF),
            dma((6,)),
            pltpu.VMEM((pool_local, tokens, half), BF),
            pltpu.VMEM((pool_local, feats, block), BF),
            pltpu.VMEM((rows, CAP, tokens, half), BF),
            pltpu.VMEM((rows, feats, block), BF),
            pltpu.VMEM((rows, CAP, tokens, half), BF),
            pltpu.VMEM((rows, feats, block), BF),
            pltpu.VMEM((8, 128), jnp.int32),
            pltpu.VMEM((8, 128), jnp.int32),
            pltpu.VMEM((rows, 128), jnp.int32),
            pltpu.VMEM((rows, 128), jnp.int32),
            pltpu.VMEM((rows, 8, 128), jnp.int32),
            pltpu.SMEM((rows, 128), jnp.int32),
            pltpu.SMEM((8, 128), jnp.int32),
            pltpu.SMEM(block_list.shape, jnp.int32),
            pltpu.SMEM(block_slot.shape, jnp.int32),
            dma((2,)),
            dma((2,)),
            pltpu.SemaphoreType.REGULAR((2,)),
            dma((2,)),
            dma((2,)),
            dma((rows,)),
            dma((rows,)),
            dma((rows,)),
            dma((rows,)),
            dma((rows,)),
            dma((rows,)),
            dma((heads,)),
            dma((carriers,)),
            dma((heads,)),
            dma((carriers,)),
            dma((carriers,)),
            dma((carriers,)),
            dma((carriers,)),
            dma((carriers,)),
            dma((2,)),
            dma((2,)),
        ],
        compiler_params=pltpu.CompilerParams(
            collective_id=0, has_side_effects=True, vmem_limit_bytes=62 << 20
        ),
        name="fused",
    )(
        block_list,
        block_slot,
        pool_latent,
        pool_rope,
        new_latent,
        new_rope,
        prefix_len,
        q_nope,
        q_rope,
        w_uk,
        w_uv,
    )


def solution(mesh):
    placed = (
        P(("groups", "req", "sub"), "head"),
        P(("groups", "req", "sub"), "head"),
        P(("groups", "req", "sub"), None),
        P(("groups", "req", "sub"), None),
        P(("groups", "req"), None, "sub"),
        P(("groups", "req"), None, None),
        P(None, "head"),
        P(None, "head"),
        P(("groups", "req"), None),
        P(("groups", "req")),
        P("groups"),
    )
    return jax.shard_map(
        shards,
        mesh=mesh,
        in_specs=placed,
        out_specs=P(("groups", "req", "sub"), "head"),
        check_vma=False,
    )
```

```python
import functools
import math

import jax
import jax.numpy as jnp
from jax import lax
from jax.experimental import pallas as pl
from jax.experimental.pallas import tpu as pltpu
from jax.sharding import PartitionSpec as P

NOPE = 128
ROPE = 64
VDIM = 128
CAP = 2
EARLY = 4
MESH = pl.DeviceIdType.MESH
BF = jnp.bfloat16
F32 = jnp.float32


def exchange(
    blocks,
    pool_local,
    scale,
    list_hbm,
    slot_hbm,
    pool_lat,
    pool_rope,
    new_lat,
    new_rope,
    length_ref,
    q_nope,
    q_rope,
    w_uk,
    w_uv,
    out,
    lat_mine,
    lat_other,
    rope_mine,
    rope_other,
    new_lat_other,
    new_rope_other,
    new_lat_v,
    new_rope_v,
    keys,
    rope_even,
    rope_odd,
    bias,
    q_nope_v,
    q_rope_v,
    w_uk_v,
    w_uv_v,
    load_sem,
    pool_l,
    pool_r,
    send_l,
    send_r,
    got_l,
    got_r,
    own_v,
    near_v,
    table_in,
    table_out,
    asked_v,
    table_s,
    asked_s,
    list_ref,
    slot_ref,
    pool_sem,
    small_sem,
    hello_sem,
    near_sem,
    table_sem,
    ask_send,
    ask_recv,
    lat_send,
    lat_recv,
    rope_send,
    rope_recv,
    xlat_send,
    xlat_recv,
    xrope_send,
    xrope_recv,
    slat_send,
    slat_recv,
    srope_send,
    srope_recv,
    snew_send,
    snew_recv,
):
    rows = lax.axis_size("req")
    heads = lax.axis_size("head")
    row = lax.axis_index("req")
    lane = lax.axis_index("head")
    core = lax.axis_index("sub")
    other = {"sub": 1 - core}
    carriers = heads
    tokens = pool_l.shape[1]
    feats = pool_r.shape[1]
    part = lane
    turn = jnp.where((lane == 0) & (core == 0), 1, 0)
    place = lax.rem(row + rows - turn, rows)

    def at(p):
        return lax.rem(p + turn, rows)

    token_at = pl.multiple_of(part * tokens, tokens)
    feat_at = pl.multiple_of(part * feats, feats)
    barrier = pltpu.get_barrier_semaphore()

    for step in range(1, heads):
        pl.semaphore_signal(
            barrier, inc=1, device_id={"head": lax.rem(lane + step, heads)}, device_id_type=MESH
        )
    pl.semaphore_signal(barrier, inc=1, device_id=other, device_id_type=MESH)

    def tell(p, carry):
        pl.semaphore_signal(barrier, inc=1, device_id={"req": at(p)}, device_id_type=MESH)
        return carry

    lax.fori_loop(place + 1, rows, tell, 0)

    load_l = pltpu.make_async_copy(
        pool_lat.at[:, pl.ds(token_at, tokens), :], pool_l, pool_sem.at[0]
    )
    load_r = pltpu.make_async_copy(
        pool_rope.at[:, pl.ds(feat_at, feats), :], pool_r, pool_sem.at[1]
    )

    load_l.start()
    load_r.start()
    loads = [
        pltpu.make_async_copy(src, dst, load_sem.at[i])
        for i, (src, dst) in enumerate(
            (
                (new_lat, new_lat_v),
                (new_rope, new_rope_v),
                (w_uk, w_uk_v),
                (q_nope, q_nope_v),
                (q_rope, q_rope_v),
                (w_uv, w_uv_v),
            )
        )
    ]
    for load in loads:
        load.start()

    to_list = pltpu.make_async_copy(list_hbm, list_ref, small_sem.at[0])
    to_slot = pltpu.make_async_copy(slot_hbm, slot_ref, small_sem.at[1])
    to_list.start()
    to_slot.start()
    to_list.wait()
    to_slot.wait()
    physical = [slot_ref[list_ref[0, j]] for j in range(blocks)]
    column = lax.broadcasted_iota(jnp.int32, own_v.shape, 1)
    own = jnp.zeros(own_v.shape, jnp.int32)
    for j in range(blocks):
        own = jnp.where(column == j, physical[j], own)
    own_v[...] = own

    @pl.when(place > 0)
    def _():
        pl.semaphore_wait(barrier, heads + place)

    def lat_copy(p, sem_at):
        return pltpu.make_async_remote_copy(
            send_l.at[p], got_l.at[row], lat_send.at[p], lat_recv.at[sem_at], {"req": p}, MESH
        )

    def rope_copy(p, sem_at):
        return pltpu.make_async_remote_copy(
            send_r.at[p], got_r.at[row], rope_send.at[p], rope_recv.at[sem_at], {"req": p}, MESH
        )

    def ask_copy(p):
        return pltpu.make_async_remote_copy(
            own_v, asked_v.at[row], ask_send.at[p], ask_recv.at[row], {"req": p}, MESH
        )

    def chosen(read):
        count = jnp.int32(0)
        first = jnp.int32(0)
        second = jnp.int32(0)
        for j in range(blocks):
            where = read(j)
            local = where - row * pool_local
            here = (local >= 0) & (local < pool_local)
            first = jnp.where(here & (count == 0), local, first)
            second = jnp.where(here & (count == 1), local, second)
            count = count + here.astype(jnp.int32)
        return first, second

    def serve(p, read):
        first, second = chosen(read)
        send_l[p, 0] = pool_l[first]
        send_l[p, 1] = pool_l[second]
        send_r[p] = pool_r[jnp.where(core == 0, first, second)]
        lat_copy(p, row).start()
        rope_copy(p, row).start()

    table_copy = pltpu.make_async_remote_copy(
        table_out,
        table_in,
        table_sem.at[0],
        table_sem.at[1],
        {"req": at(lax.rem(place + 2, rows))},
        MESH,
    )
    near_copy = pltpu.make_async_remote_copy(
        own_v, near_v, near_sem.at[0], near_sem.at[1], {"req": at(lax.rem(place + 1, rows))}, MESH
    )

    for step in (1, 2):

        @pl.when(place >= step)
        def _(step=step):
            pl.semaphore_signal(
                hello_sem.at[step - 1],
                inc=1,
                device_id={"req": at(place - step)},
                device_id_type=MESH,
            )

    def ask(p, carry):
        ask_copy(at(p)).start()
        return carry

    lax.fori_loop(0, place, ask, 0)
    load_l.wait()
    load_r.wait()

    @pl.when(place < rows - 1)
    def _():
        pl.semaphore_wait(hello_sem.at[0], 1)
        near_copy.start()

    @pl.when(place > 1)
    def _():
        table_copy.wait_recv()

    @pl.when(place > 0)
    def _():
        near_copy.wait_recv()

    line = lax.broadcasted_iota(jnp.int32, table_out.shape, 0)
    line_place = lax.rem(line + rows - turn, rows)
    mine = jnp.broadcast_to(own_v[0:1, :], table_out.shape)
    near = jnp.broadcast_to(near_v[0:1, :], table_out.shape)
    known = jnp.where(line_place < place - 1, table_in[...], 0)
    known = jnp.where(line_place == place - 1, near, known)
    table_out[...] = jnp.where(line == row, mine, known)

    def below(p, carry):
        r = at(p)
        serve(r, lambda j: table_s[r, j])
        return carry

    early = jnp.minimum(place, EARLY)

    @pl.when(place > 0)
    def _():
        to_s = pltpu.make_async_copy(table_out, table_s, small_sem.at[0])
        to_s.start()
        to_s.wait()
        lax.fori_loop(0, early, below, 0)

    @pl.when(place < rows - 2)
    def _():
        pl.semaphore_wait(hello_sem.at[1], 1)
        table_copy.start()

    lax.fori_loop(early, place, below, 0)

    fresh_rows = q_nope.shape[0]
    ahead_rows = blocks * lat_mine.shape[1]
    key = lax.broadcasted_iota(jnp.int32, (fresh_rows, keys.shape[0]), 1)
    query = lax.broadcasted_iota(jnp.int32, (fresh_rows, keys.shape[0]), 0)
    last = jnp.where(core == 1, keys.shape[0], ahead_rows + fresh_rows)
    hidden = F32(-1e30)
    in_prefix = jnp.where(key < length_ref[0], F32(0.0), hidden)
    in_mine = jnp.where(key - ahead_rows <= query, F32(0.0), hidden)
    in_other = jnp.where(key < last, F32(0.0), hidden)
    fresh = jnp.where(key < ahead_rows + fresh_rows, in_mine, in_other)
    bias[...] = jnp.where(key < ahead_rows, in_prefix, fresh)

    @pl.when(place < rows - 1)
    def _():

        def above(p, carry):
            r = at(p)
            pltpu.make_async_remote_copy(
                own_v, asked_v.at[r], ask_send.at[r], ask_recv.at[r], {"req": r}, MESH
            ).wait_recv()
            to_s = pltpu.make_async_copy(asked_v.at[r], asked_s, small_sem.at[1])
            to_s.start()
            to_s.wait()
            serve(r, lambda j: asked_s[0, j])
            return carry

        lax.fori_loop(place + 1, rows, above, 0)

    first, second = chosen(lambda j: physical[j])
    got_l[row, 0] = pool_l[first]
    got_l[row, 1] = pool_l[second]
    got_r[row] = pool_r[jnp.where(core == 0, first, second)]

    def arrived(p, carry):
        @pl.when(p != row)
        def _():
            lat_copy(p, p).wait_recv()
            rope_copy(p, p).wait_recv()

        return carry

    lax.fori_loop(0, rows, arrived, 0)

    for j in range(blocks):
        owner = physical[j] // pool_local
        rank = jnp.int32(0)
        for i in range(j):
            rank = rank + (physical[i] // pool_local == owner).astype(jnp.int32)
        lat_mine[j, pl.ds(token_at, tokens), :] = got_l[owner, jnp.minimum(rank, CAP - 1)]
        piece = got_r[owner]
        rope_mine[j, pl.ds(feat_at, feats), :] = jnp.where(
            rank == core, piece, jnp.zeros_like(piece)
        )

    @pl.when(place == 0)
    def _():
        pl.semaphore_wait(barrier, heads)

    for load in loads:
        load.wait()
    new_copies = [
        pltpu.make_async_remote_copy(
            src, dst, snew_send.at[i], snew_recv.at[i], other, MESH
        )
        for i, (src, dst) in enumerate(((new_lat_v, new_lat_other), (new_rope_v, new_rope_other)))
    ]
    for copy in new_copies:
        copy.start()

    def lat_piece(k):
        return pl.ds(pl.multiple_of(k * tokens, tokens), tokens)

    def rope_piece(k):
        return pl.ds(pl.multiple_of(k * feats, feats), feats)

    def xlat_copy(k, peer):
        at = lat_piece(k)
        return pltpu.make_async_remote_copy(
            lat_mine.at[:, at, :],
            lat_mine.at[:, at, :],
            xlat_send.at[peer],
            xlat_recv.at[k],
            {"head": peer},
            MESH,
        )

    def xrope_copy(k, peer):
        at = rope_piece(k)
        return pltpu.make_async_remote_copy(
            rope_mine.at[:, at, :],
            rope_mine.at[:, at, :],
            xrope_send.at[peer],
            xrope_recv.at[k],
            {"head": peer},
            MESH,
        )

    def sub_copies(k):
        at, fat = lat_piece(k), rope_piece(k)
        return (
            pltpu.make_async_remote_copy(
                lat_mine.at[:, at, :],
                lat_other.at[:, at, :],
                slat_send.at[k],
                slat_recv.at[k],
                other,
                MESH,
            ),
            pltpu.make_async_remote_copy(
                rope_mine.at[:, fat, :],
                rope_other.at[:, fat, :],
                srope_send.at[k],
                srope_recv.at[k],
                other,
                MESH,
            ),
        )

    order = [0]
    for step in range(heads // 2, 0, -1):
        for peer in (step, heads - step):
            if peer not in order:
                order.append(peer)
    order = order[1:]

    for step in order:
        peer = lax.rem(lane + step, heads)
        xlat_copy(part, peer).start()
        xrope_copy(part, peer).start()
    for copy in sub_copies(part):
        copy.start()

    for k in range(carriers):

        @pl.when(part != k)
        def _(k=k):
            xlat_copy(k, lane).wait_recv()
            xrope_copy(k, lane).wait_recv()
            for copy in sub_copies(k):
                copy.start()

    for k in range(carriers):
        for copy in sub_copies(k):
            copy.wait()
    for copy in new_copies:
        copy.wait()

    blocks, block, half = lat_mine.shape
    prefix = blocks * block
    queries = q_nope.shape[0]
    total = keys.shape[0]
    here = pl.ds(pl.multiple_of(core * half, half), half)
    there = pl.ds(pl.multiple_of((1 - core) * half, half), half)
    for j in range(blocks):
        keys[pl.ds(j * block, block), here] = lat_mine[j]
        keys[pl.ds(j * block, block), there] = lat_other[j]
    keys[pl.ds(prefix, queries), :] = new_lat_v[...]
    keys[pl.ds(prefix + queries, queries), :] = new_lat_other[...]

    def put_rope(at, piece):
        turned = piece.astype(F32).T.astype(BF)
        blank = jnp.zeros_like(turned)
        rope_even[pl.ds(at, turned.shape[0]), :] = jnp.concatenate([turned, blank], axis=1)
        rope_odd[pl.ds(at, turned.shape[0]), :] = jnp.concatenate([blank, turned], axis=1)

    for j in range(blocks):
        put_rope(j * block, rope_mine[j] + rope_other[j])
    put_rope(prefix, new_rope_v[...])
    put_rope(prefix + queries, new_rope_other[...])

    def pair(i, carry):
        cols = pl.ds(pl.multiple_of(i * 2 * NOPE, 2 * NOPE), 2 * NOPE)
        k2 = jnp.dot(keys[...], w_uk_v[:, cols], preferred_element_type=F32).astype(BF)
        v2 = jnp.dot(keys[...], w_uv_v[:, cols], preferred_element_type=F32).astype(BF)
        qr = q_rope_v[:, pl.ds(pl.multiple_of(i * 2 * ROPE, 2 * ROPE), 2 * ROPE)]
        qn = q_nope_v[:, cols]
        outs = []
        for e, kr in ((0, rope_even), (1, rope_odd)):
            kcat = jnp.concatenate([k2[:, e * NOPE : (e + 1) * NOPE], kr[...]], axis=1)
            qcat = jnp.concatenate([qn[:, e * NOPE : (e + 1) * NOPE], qr], axis=1)
            s = lax.dot_general(
                qcat, kcat, (((1,), (1,)), ((), ())), preferred_element_type=F32
            )
            s = s * scale + bias[...]
            peak = jnp.max(s, axis=1, keepdims=True)
            expo = jnp.exp(s - peak)
            weights = (expo * (1.0 / jnp.sum(expo, axis=1, keepdims=True))).astype(BF)
            outs.append(
                jnp.dot(
                    weights, v2[:, e * VDIM : (e + 1) * VDIM], preferred_element_type=F32
                ).astype(BF)
            )
        out[:, cols] = jnp.concatenate(outs, axis=1)
        return carry

    lax.fori_loop(0, q_nope.shape[1] // (2 * NOPE), pair, 0, unroll=True)

    for step in order:
        peer = lax.rem(lane + step, heads)
        xlat_copy(part, peer).wait_send()
        xrope_copy(part, peer).wait_send()

    def sent(p, carry):
        r = at(p)

        @pl.when(p != place)
        def _():
            lat_copy(r, row).wait_send()
            rope_copy(r, row).wait_send()

        @pl.when(p < place)
        def _():
            ask_copy(r).wait_send()

        return carry

    lax.fori_loop(0, rows, sent, 0)

    @pl.when(place < rows - 1)
    def _():
        near_copy.wait_send()

    @pl.when(place < rows - 2)
    def _():
        table_copy.wait_send()


def shards(
    q_nope,
    q_rope,
    new_latent,
    new_rope,
    pool_latent,
    pool_rope,
    w_uk,
    w_uv,
    block_list,
    prefix_len,
    block_slot,
):
    rows = lax.axis_size("req")
    heads = lax.axis_size("head")
    pool_local, block, half = pool_latent.shape
    blocks = block_list.shape[1]
    queries = q_nope.shape[0]
    carriers = heads
    tokens = block // carriers
    feats = ROPE // carriers
    pool_rope = jnp.swapaxes(pool_rope, 1, 2)
    new_rope = new_rope.T
    vmem = pl.BlockSpec(memory_space=pltpu.VMEM)
    smem = pl.BlockSpec(memory_space=pltpu.SMEM)
    hbm = pl.BlockSpec(memory_space=pltpu.HBM)
    dma = pltpu.SemaphoreType.DMA
    shape = jax.ShapeDtypeStruct
    total = (blocks * block) + 2 * queries
    return pl.pallas_call(
        functools.partial(exchange, blocks, pool_local, 1.0 / math.sqrt(NOPE + ROPE)),
        out_shape=shape(q_nope.shape, BF),
        in_specs=[hbm] * 6 + [smem] + [hbm] * 4,
        out_specs=vmem,
        scratch_shapes=[
            pltpu.VMEM((blocks, block, half), BF),
            pltpu.VMEM((blocks, block, half), BF),
            pltpu.VMEM((blocks, ROPE, block), BF),
            pltpu.VMEM((blocks, ROPE, block), BF),
            pltpu.VMEM(new_latent.shape, BF),
            pltpu.VMEM(new_rope.shape, BF),
            pltpu.VMEM(new_latent.shape, BF),
            pltpu.VMEM(new_rope.shape, BF),
            pltpu.VMEM((total, 2 * half), BF),
            pltpu.VMEM((total, 2 * ROPE), BF),
            pltpu.VMEM((total, 2 * ROPE), BF),
            pltpu.VMEM((queries, total), F32),
            pltpu.VMEM(q_nope.shape, BF),
            pltpu.VMEM(q_rope.shape, BF),
            pltpu.VMEM(w_uk.shape, BF),
            pltpu.VMEM(w_uv.shape, BF),
            dma((6,)),
            pltpu.VMEM((pool_local, tokens, half), BF),
            pltpu.VMEM((pool_local, feats, block), BF),
            pltpu.VMEM((rows, CAP, tokens, half), BF),
            pltpu.VMEM((rows, feats, block), BF),
            pltpu.VMEM((rows, CAP, tokens, half), BF),
            pltpu.VMEM((rows, feats, block), BF),
            pltpu.VMEM((8, 128), jnp.int32),
            pltpu.VMEM((8, 128), jnp.int32),
            pltpu.VMEM((rows, 128), jnp.int32),
            pltpu.VMEM((rows, 128), jnp.int32),
            pltpu.VMEM((rows, 8, 128), jnp.int32),
            pltpu.SMEM((rows, 128), jnp.int32),
            pltpu.SMEM((8, 128), jnp.int32),
            pltpu.SMEM(block_list.shape, jnp.int32),
            pltpu.SMEM(block_slot.shape, jnp.int32),
            dma((2,)),
            dma((2,)),
            pltpu.SemaphoreType.REGULAR((2,)),
            dma((2,)),
            dma((2,)),
            dma((rows,)),
            dma((rows,)),
            dma((rows,)),
            dma((rows,)),
            dma((rows,)),
            dma((rows,)),
            dma((heads,)),
            dma((carriers,)),
            dma((heads,)),
            dma((carriers,)),
            dma((carriers,)),
            dma((carriers,)),
            dma((carriers,)),
            dma((carriers,)),
            dma((2,)),
            dma((2,)),
        ],
        compiler_params=pltpu.CompilerParams(
            collective_id=0, has_side_effects=True, vmem_limit_bytes=62 << 20
        ),
        name="fused",
    )(
        block_list,
        block_slot,
        pool_latent,
        pool_rope,
        new_latent,
        new_rope,
        prefix_len,
        q_nope,
        q_rope,
        w_uk,
        w_uv,
    )


def solution(mesh):
    placed = (
        P(("groups", "req", "sub"), "head"),
        P(("groups", "req", "sub"), "head"),
        P(("groups", "req", "sub"), None),
        P(("groups", "req", "sub"), None),
        P(("groups", "req"), None, "sub"),
        P(("groups", "req"), None, None),
        P(None, "head"),
        P(None, "head"),
        P(("groups", "req"), None),
        P(("groups", "req")),
        P("groups"),
    )
    return jax.shard_map(
        shards,
        mesh=mesh,
        in_specs=placed,
        out_specs=P(("groups", "req", "sub"), "head"),
        check_vma=False,
    )
```
